32 devices in a mesh: dp: 4 (over x, core), expert: 8 (over z, y).
Axes of the slice: x: 2, y: 2, z: 4, core: 2. Of those that a mesh axis runs over, the one named last changes fastest.
Arguments:
- tokens: bfloat16 [4096, 2048], P(('dp', 'expert')), may hold values from -6 to 6
- norm_gain: bfloat16 [2048], replicated, may hold values from 0.099609375 to 1.8984375
- router_weight: bfloat16 [2048, 8], replicated, may hold values from -0.1875 to 0.1875
- w_gate: bfloat16 [8, 2048, 5120], P('expert', None, 'dp'), may hold values from -0.125 to 0.125
- w_up: bfloat16 [8, 2048, 5120], P('expert', None, 'dp'), may hold values from -0.125 to 0.125
- w_down: bfloat16 [8, 5120, 2048], P('expert', 'dp'), may hold values from -0.078125 to 0.078125
- selected: int32 [8, 896], replicated, may hold values from 0 to 4095, as said below
Outputs:
- combined: bfloat16 [4096, 2048], P(('dp', 'expert'))
The draws below stay inside these ranges and needn't reach their ends.
Inputs may be any that keep to these rules, and one draw needn't show every extreme that they name: `selected`: each row holds 896 distinct token indices in ascending order. Of one row's indices at most 64 fall among one device's 128 tokens and at most 336 among the tokens of one index of dp; every row reaches both bounds.
All inputs are finite; a program needn't handle non-finite values.
Results may differ from the reference program's by a relative error of at most 0.0072.
Values may be sent and summed in bfloat16 or wider, within the bound.
A program may use at most 128 MiB of HBM per device.

```python
import jax
import jax.numpy as jnp
from jax import lax

D = 2048
FF = 5120
TOK_DEV = 128
EXPERTS = 8
TOKENS = 4096
CAP = 896
PEAK = 64
RMOST = 336
N_DP = 4
N_EXPERT = 8


def choose_tokens(key):
    keys = jax.random.split(key, 7)
    row_cells = N_DP * RMOST
    row_score = jax.random.randint(keys[0], (N_DP, RMOST), 0, 1024) + 1024 * jax.random.randint(keys[1], (N_DP, 1), 0, 16)
    forced_row = jax.random.randint(keys[2], (), 0, N_DP)
    row_score = row_score + jnp.where(jnp.arange(N_DP) == forced_row, 32768, 0)[:, None]
    row_distinct = row_score.reshape(-1) * row_cells + jnp.arange(row_cells)
    row_order = jnp.argsort(-row_distinct)
    row_ranks = jnp.argsort(row_order)
    row_counts = jnp.sum((row_ranks < CAP).reshape(N_DP, RMOST).astype(jnp.int32), axis=1)
    source_cells = N_EXPERT * PEAK
    source_score = jax.random.randint(keys[3], (N_DP, N_EXPERT, PEAK), 0, 1024) + 1024 * jax.random.randint(keys[4], (N_DP, N_EXPERT, 1), 0, 16)
    forced_source = jax.random.randint(keys[5], (N_DP,), 0, N_EXPERT)
    source_score = source_score + jnp.where(jnp.arange(N_EXPERT)[None, :] == forced_source[:, None], 32768, 0)[:, :, None]
    source_distinct = source_score.reshape(N_DP, source_cells) * source_cells + jnp.arange(source_cells)[None, :]
    source_order = jnp.argsort(-source_distinct, axis=1)
    source_ranks = jnp.argsort(source_order, axis=1)
    chosen_cells = source_ranks < row_counts[:, None]
    source_counts = jnp.sum(chosen_cells.reshape(N_DP, N_EXPERT, PEAK).astype(jnp.int32), axis=2).reshape(-1)
    shuffled = jnp.argsort(jax.random.randint(keys[6], (N_DP * N_EXPERT, TOK_DEV), 0, 1073741824), axis=1)[:, :PEAK]
    candidates = jnp.arange(N_DP * N_EXPERT)[:, None] * TOK_DEV + shuffled
    usable = jnp.arange(PEAK)[None, :] < source_counts[:, None]
    sort_keys = jnp.where(usable, candidates, N_DP * N_EXPERT * TOK_DEV).reshape(-1)
    return jnp.sort(sort_keys)[:CAP].astype(jnp.int32)


def draw_selected(key, part):
    expert_keys = jax.random.split(jax.random.fold_in(key, 17), EXPERTS)
    return jax.vmap(choose_tokens)(expert_keys)


def levels(key, dims, cuts, low, largest):
    gain, own = 1.0, jax.random.fold_in(key, 6)
    for axis_at, blocks in cuts:
        draws = jnp.exp(jax.random.uniform(jax.random.fold_in(own, axis_at), (blocks,), jnp.float32, low / len(cuts), largest / len(cuts)))
        gain = gain * jnp.repeat(draws, dims[axis_at] // blocks).reshape([-1 if axis == axis_at else 1 for axis in range(len(dims))])
    return gain


def normal_values(own_key, dims, width, bound, shards=(), dtype=jnp.bfloat16):
    values = jax.random.normal(own_key, dims, jnp.float32) * width
    if len(shards) > 0:
        values = levels(own_key, dims, shards, -0.22, 0.18) * values
    return jnp.clip(values, min=-bound, max=bound).astype(dtype)


def setup_inputs(seed: int = 0) -> dict:
    seeds = jax.random.split(jax.random.key(seed), 8)
    tokens = normal_values(seeds[0], (TOKENS, D), 1.0, 6.0, ((0, 32),))
    norm_gain = jnp.clip(1.0 + 0.18 * jax.random.normal(seeds[1], (D,), jnp.float32), 0.099609375, 1.8984375).astype(jnp.bfloat16)
    router_weight = normal_values(seeds[2], (D, EXPERTS), (D // 2) ** -0.5, 0.1875)
    w_gate = normal_values(seeds[3], (EXPERTS, D, FF), D ** -0.5, 0.125, ((0, 8), (2, 4)))
    w_up = normal_values(seeds[4], (EXPERTS, D, FF), D ** -0.5, 0.125, ((0, 8), (2, 4)))
    w_down = normal_values(seeds[5], (EXPERTS, FF, D), FF ** -0.5, 0.078125, ((0, 8), (1, 4)))
    selected = draw_selected(jax.random.fold_in(seeds[7], 71), 0)
    return dict(tokens=tokens, norm_gain=norm_gain, router_weight=router_weight, w_gate=w_gate, w_up=w_up, w_down=w_down, selected=selected)


def reference(tokens, norm_gain, router_weight, w_gate, w_up, w_down, selected):
    activations = tokens.astype(jnp.float32)
    mean_square = lax.optimization_barrier(jnp.mean(activations * activations, axis=1, keepdims=True))
    normed = (activations * lax.rsqrt(mean_square + 1e-06) * norm_gain.astype(jnp.float32)).astype(jnp.bfloat16)
    gate_probs = jax.nn.sigmoid(jnp.dot(normed, router_weight, preferred_element_type=jnp.float32))
    probs_by_expert = gate_probs.T

    def per_expert(total, inputs):
        gate_matrix, up_matrix, down_matrix, chosen, probs = inputs
        expert_rows = normed[chosen]
        gate_part = jnp.dot(expert_rows, gate_matrix, preferred_element_type=jnp.float32)
        up_part = jnp.dot(expert_rows, up_matrix, preferred_element_type=jnp.float32)
        hidden = (jax.nn.gelu(gate_part, approximate=True) * up_part).astype(jnp.bfloat16)
        expert_out = jnp.dot(hidden, down_matrix, preferred_element_type=jnp.float32).astype(jnp.bfloat16)
        weights = probs[chosen]
        total = total.at[chosen].add(weights[:, None] * expert_out.astype(jnp.float32))
        return (total, None)
    start = jnp.zeros(normed.shape, jnp.float32)
    total, unused = lax.scan(per_expert, start, (w_gate, w_up, w_down, selected.astype(jnp.int32), probs_by_expert))
    return total.astype(jnp.bfloat16)
```

```python
import functools

import jax
import jax.numpy as jnp
from jax import lax
from jax.experimental import pallas as pl
from jax.experimental.pallas import tpu as pltpu
from jax.sharding import PartitionSpec as P

MESH = pl.DeviceIdType.MESH
F32 = jnp.float32
BF16 = jnp.bfloat16
CHUNKS = 8
AHEAD = 2
NEAR_LAG, CHIP_LAG, CORE_LAG = 2, 2, 1
SIB_LAG, X_LAG, BACK_LAG, PAIR_LAG = 1, 2, 2, 2


def tile_of(width):
    for tile in (256, 128):
        if width % tile == 0:
            return tile
    return width


def remote(src, dst, send_sem, recv_sem, **where):
    return pltpu.make_async_remote_copy(
        src_ref=src,
        dst_ref=dst,
        send_sem=send_sem,
        recv_sem=recv_sem,
        device_id=where,
        device_id_type=MESH,
    )


def iota(shape, axis):
    return lax.broadcasted_iota(jnp.int32, shape, axis)


def kernel(
    experts, chips, chunks,
    tokens_hbm, gain_hbm, router_hbm, selected_hbm, wg_hbm, wu_hbm, wd_hbm, out,
    tokens, gain, router, selected, chosen, pick, pack, unpack, mix_high, mix_low,
    tok_out, tok_in, outgoing, received, rows, wg, wu, wd, acc_g, acc_u, hidden,
    sib_in, x_in, returning, arrived, back_out, back_in,
    i_sem, w_sem, d_sem, t_send, t_recv, a_send, a_recv, x_send, s_send, b_recv,
    c_send, c_recv, o_send, o_recv, r_send, r_recv, p_send, p_recv,
):
    half = experts // 2
    dp_count = 2 * chips
    tok_rows = tokens.shape[0]
    width = tok_out.shape[2]
    slots = received.shape[2]
    room = rows.shape[2]
    capacity = selected.shape[1]
    ff = wg.shape[1]
    tile = tile_of(ff)
    lanes = half * slots

    me = lax.axis_index("expert")
    dp = lax.axis_index("dp")
    chip, core = dp // 2, dp % 2
    base, local = (me // half) * half, me % half
    partner = (me + half) % experts
    sibling = 2 * chip + 1 - core

    loads = [
        pltpu.make_async_copy(src, dst, i_sem.at[i])
        for i, (src, dst) in enumerate(
            (
                (tokens_hbm, tokens),
                (gain_hbm, gain),
                (selected_hbm, selected.at[pl.ds(0, experts)]),
                (router_hbm, router),
            )
        )
    ]
    for copy in loads:
        copy.start()

    barrier = pltpu.get_barrier_semaphore()

    def expert_hello(i, carry):
        pl.semaphore_signal(
            barrier, inc=1, device_id={"expert": base + (local + i) % half}, device_id_type=MESH
        )
        return carry

    lax.fori_loop(1, half, expert_hello, 0)
    pl.semaphore_signal(barrier, inc=1, device_id={"expert": partner}, device_id_type=MESH)
    pl.semaphore_signal(barrier, inc=1, device_id={"dp": sibling}, device_id_type=MESH)
    for i in range(1, chips):
        pl.semaphore_signal(
            barrier,
            inc=1,
            device_id={"dp": 2 * ((chip + i) % chips) + core},
            device_id_type=MESH,
        )

    def weights(k):
        part = pl.ds(k * width, width)
        return (
            pltpu.make_async_copy(wg_hbm.at[part], wg.at[part], w_sem.at[k, 0]),
            pltpu.make_async_copy(wu_hbm.at[part], wu.at[part], w_sem.at[k, 1]),
        )

    def down_weights(k):
        part = pl.ds(k * width, width)
        return pltpu.make_async_copy(wd_hbm.at[:, part], wd.at[k], d_sem.at[k])

    loads[0].wait()
    loads[1].wait()
    for k in range(chunks):
        for copy in weights(k):
            copy.start()
    for k in range(chunks):
        down_weights(k).start()
    activations = tokens[...].astype(F32)
    mean_square = jnp.mean(activations * activations, axis=1, keepdims=True)
    scale = lax.rsqrt(mean_square + 1e-06)
    for k in range(chunks):
        part = slice(k * width, (k + 1) * width)
        tok_out[k] = (
            tokens[:, part].astype(F32) * scale * gain[:, part].astype(F32)
        ).astype(BF16)
    pl.semaphore_wait(barrier, half + chips)

    def to_partner(k):
        return remote(
            tok_out.at[k], tok_in.at[k], t_send.at[k], t_recv.at[k], expert=partner
        )

    def to_expert(k, side, i):
        near = (local + i) % half
        owner = (me + side * half) % experts
        return remote(
            outgoing.at[k, side, near], received.at[k, owner],
            a_send.at[k, side, near], a_recv.at[k, owner], expert=base + near,
        )

    def from_expert(k, side, i):
        near = (local + i) % half
        owner = (base + near + side * half) % experts
        return remote(
            outgoing.at[k, side, near], received.at[k, owner],
            a_send.at[k, side, near], a_recv.at[k, owner], expert=base + near,
        )

    def to_chip(k, i):
        other = 2 * ((chip + i) % chips) + core
        return remote(
            rows.at[k, dp], rows.at[k, dp], x_send.at[k, i], b_recv.at[k, dp], dp=other
        )

    def from_chip(k, i):
        other = 2 * ((chip + i) % chips) + core
        return remote(
            rows.at[k, other], rows.at[k, other], x_send.at[k, i], b_recv.at[k, other], dp=other
        )

    def to_sibling(k, i):
        block = 2 * ((chip + i) % chips) + core
        return remote(
            rows.at[k, block], rows.at[k, block], s_send.at[k, i], b_recv.at[k, block],
            dp=sibling,
        )

    def from_sibling(k, i):
        block = 2 * ((chip + i) % chips) + 1 - core
        return remote(
            rows.at[k, block], rows.at[k, block], s_send.at[k, i], b_recv.at[k, block],
            dp=sibling,
        )

    for k in range(min(AHEAD, chunks)):
        to_partner(k).start()
    loads[2].wait()
    loads[3].wait()

    spot = iota((1, capacity), 1).astype(F32)
    lane = iota((1, lanes), 1).astype(F32)

    def choose(side):
        first = (dp * experts + (me + side * half) % experts) * tok_rows
        ids = first + iota((tok_rows, 1), 0)
        total = jnp.zeros((tok_rows, lanes), F32)
        for e in range(half):
            row = selected[pl.ds(base + e, 1), :]
            at = jnp.max(jnp.where(row == ids, spot, -1.0), axis=1, keepdims=True)
            begin = jnp.sum(jnp.where(row < first, 1.0, 0.0), axis=1, keepdims=True)
            goal = jnp.where(at >= 0.0, at - begin + float(e * slots), -1.0)
            total = total + jnp.where(goal == lane, 1.0, 0.0)
        chosen[side] = total.astype(BF16)
        pick[side] = total.T.astype(BF16)

    def send_rows(k, side, source):
        picked = jnp.dot(pick[side], source, preferred_element_type=F32)
        outgoing[k, side] = picked.astype(BF16).reshape(half, slots, width)

        def send(i, carry):
            to_expert(k, side, i).start()
            return carry

        lax.fori_loop(1, half, send, 0)
        received[k, (me + side * half) % experts] = outgoing[k, side, local]

    choose(0)
    send_rows(0, 0, tok_out[0])
    choose(1)

    mine = selected[pl.ds(me, 1), :]
    starts = (dp * experts + iota((experts + 8, 1), 0)) * tok_rows
    firsts = jnp.sum(jnp.where(mine < starts, 1.0, 0.0), axis=1, keepdims=True)
    place = iota((1, experts * slots), 1).astype(F32)
    target = jnp.full((1, experts * slots), -1.0, F32)
    slot = iota((slots, 1), 0).astype(F32)
    seats = iota((1, room), 1).astype(F32)
    for j in range(experts):
        offset = firsts[j : j + 1] - firsts[0:1]
        count = firsts[j + 1 : j + 2] - firsts[j : j + 1]
        within = place - float(j * slots)
        here = jnp.logical_and(within >= 0.0, within < count)
        target = jnp.where(here, within + offset, target)
        goal = jnp.where(slot < count, slot + offset, -1.0)
        unpack[j * slots : (j + 1) * slots, :] = jnp.where(goal == seats, 1.0, 0.0).astype(BF16)
    seat = iota((room, 1), 0).astype(F32)
    pack[...] = jnp.where(seat == target, 1.0, 0.0).astype(BF16)

    def weigh(side, source):
        logits = jnp.zeros((tok_rows, experts), F32)
        for k in range(chunks):
            logits = logits + lax.dot_general(
                source[k], router[:, k * width : (k + 1) * width],
                (((1,), (1,)), ((), ())), preferred_element_type=F32,
            )
        probs = jax.nn.sigmoid(logits)
        column = iota((1, experts), 1)
        spread = jnp.zeros((tok_rows, lanes), F32)
        for e in range(half):
            prob = jnp.sum(jnp.where(column == base + e, probs, 0.0), axis=1, keepdims=True)
            inside = jnp.logical_and(lane >= float(e * slots), lane < float((e + 1) * slots))
            spread = jnp.where(inside, prob, spread)
        mixing = jnp.where(chosen[side].astype(F32) > 0.5, spread, 0.0)
        high = mixing.astype(BF16)
        mix_high[side] = high
        mix_low[side] = (mixing - high.astype(F32)).astype(BF16)

    lag_x = NEAR_LAG + CHIP_LAG
    lag_m = lag_x + CORE_LAG
    for step in range(chunks + lag_m):
        if step < chunks:
            to_partner(step).wait_recv()
            send_rows(step, 1, tok_in[step])
        if step + AHEAD < chunks:
            to_partner(step + AHEAD).start()
        if step + 1 < chunks:
            send_rows(step + 1, 0, tok_out[step + 1])
        if NEAR_LAG <= step < chunks + NEAR_LAG:
            k = step - NEAR_LAG

            def take(i, carry):
                from_expert(k, 0, i).wait_recv()
                from_expert(k, 1, i).wait_recv()
                return carry

            lax.fori_loop(1, half, take, 0)
            packed = jnp.dot(
                pack[...],
                received[k].reshape(experts * slots, width),
                preferred_element_type=F32,
            )
            rows[k, dp] = packed.astype(BF16)
            for i in range(1, chips):
                to_chip(k, i).start()
            to_sibling(k, 0).start()
        if lag_x <= step < chunks + lag_x:
            k = step - lag_x
            for i in range(1, chips):
                from_chip(k, i).wait_recv()
                to_sibling(k, i).start()
        if step == chunks:
            weigh(0, tok_out)
            weigh(1, tok_in)
        if step >= lag_m:
            k = step - lag_m
            for i in range(chips):
                from_sibling(k, i).wait_recv()
            for copy in weights(k):
                copy.wait()

            def multiply(n, carry):
                cols = pl.ds(pl.multiple_of(n * tile, tile), tile)
                depth = pl.ds(k * width, width)
                block = rows[k].reshape(dp_count * room, width)
                g = jnp.dot(block, wg[depth, cols], preferred_element_type=F32)
                u = jnp.dot(block, wu[depth, cols], preferred_element_type=F32)
                if k > 0:
                    g = g + acc_g[:, cols]
                    u = u + acc_u[:, cols]
                if k < chunks - 1:
                    acc_g[:, cols] = g
                    acc_u[:, cols] = u
                else:
                    hidden[:, cols] = (jax.nn.gelu(g, approximate=True) * u).astype(BF16)
                return carry

            lax.fori_loop(0, ff // tile, multiply, 0)

    places = ff // width

    def own(k, i):
        at = k % (2 * places)
        row = ((at // places) * chips + i) * room
        return acc_g.at[pl.ds(row, room), pl.ds((at % places) * width, width)]

    def sib_copy(k, i):
        return remote(
            rows.at[k, i], sib_in.at[k, i], c_send.at[k, i], c_recv.at[k, i], dp=sibling
        )

    def chip_copy(k, i):
        return remote(
            rows.at[k, chips + i - 1], x_in.at[k, i - 1],
            o_send.at[k, i - 1], o_recv.at[k, i - 1],
            dp=2 * ((chip + i) % chips) + core,
        )

    def give_back(k, side, i):
        near = (local + i) % half
        owner = (base + near + side * half) % experts
        return remote(
            returning.at[k, owner], arrived.at[k, side, local],
            r_send.at[k, owner], r_recv.at[k, side, local], expert=base + near,
        )

    def take_back(k, side, i):
        near = (local + i) % half
        owner = (base + near + side * half) % experts
        return remote(
            returning.at[k, owner], arrived.at[k, side, near],
            r_send.at[k, owner], r_recv.at[k, side, near], expert=base + near,
        )

    def pair_copy(k):
        return remote(
            back_out.at[k], back_in.at[k], p_send.at[k], p_recv.at[k], expert=partner
        )

    def mixed(k, side):
        values = arrived[k, side].reshape(half * slots, width)
        sums = jnp.dot(mix_high[side], values, preferred_element_type=F32)
        return sums + jnp.dot(mix_low[side], values, preferred_element_type=F32)

    def take_side(k, side):
        def take(i, carry):
            take_back(k, side, i).wait_recv()
            return carry

        lax.fori_loop(1, half, take, 0)

    def block_rows(block):
        return hidden[pl.ds(pl.multiple_of(block * room, 16), room), :]

    lag_t = SIB_LAG + X_LAG
    lag_b = lag_t + BACK_LAG
    lag_p = lag_b + PAIR_LAG
    for step in range(chunks + lag_p):
        if step < chunks:
            k = step
            down_weights(k).wait()
            for i in range(1, chips):
                to_chip(k, i).wait_send()
            for i in range(chips):
                to_sibling(k, i).wait_send()

            def give(i, carry):
                block = 2 * ((chip + i) % chips) + 1 - core
                term = jnp.dot(block_rows(block), wd[k], preferred_element_type=F32)
                rows[k, i] = term.astype(BF16)
                sib_copy(k, i).start()
                return carry

            lax.fori_loop(0, chips, give, 0)

            def keep(i, carry):
                block = 2 * ((chip + i) % chips) + core
                own(k, i)[...] = jnp.dot(block_rows(block), wd[k], preferred_element_type=F32)
                return carry

            lax.fori_loop(0, chips, keep, 0)
        if SIB_LAG <= step < chunks + SIB_LAG:
            k = step - SIB_LAG
            for i in range(chips):
                sib_copy(k, i).wait_recv()
            for i in range(1, chips):
                rows[k, chips + i - 1] = (own(k, i)[...] + sib_in[k, i].astype(F32)).astype(BF16)
                chip_copy(k, i).start()
        if lag_t <= step < chunks + lag_t:
            k = step - lag_t
            total = own(k, 0)[...] + sib_in[k, 0].astype(F32)
            for i in range(1, chips):
                chip_copy(k, i).wait_recv()
                total = total + x_in[k, i - 1].astype(F32)
            spread = jnp.dot(unpack[...], total.astype(BF16), preferred_element_type=F32)
            returning[k] = spread.astype(BF16).reshape(experts, slots, width)
            for side in (1, 0):

                def send(i, carry):
                    give_back(k, side, i).start()
                    return carry

                lax.fori_loop(1, half, send, 0)
                arrived[k, side, local] = returning[k, (me + side * half) % experts]
        if lag_b <= step < chunks + lag_b:
            k = step - lag_b
            take_side(k, 1)
            back_out[k] = mixed(k, 1).astype(BF16)
            pair_copy(k).start()
        if step >= lag_p:
            k = step - lag_p
            take_side(k, 0)
            near_sum = mixed(k, 0)
            pair_copy(k).wait_recv()
            combined = near_sum + back_in[k].astype(F32)
            out[:, k * width : (k + 1) * width] = combined.astype(BF16)

    for k in range(chunks):
        to_partner(k).wait_send()

        def sent(i, carry):
            for side in (0, 1):
                to_expert(k, side, i).wait_send()
                give_back(k, side, i).wait_send()
            return carry

        lax.fori_loop(1, half, sent, 0)
        for i in range(chips):
            sib_copy(k, i).wait_send()
        for i in range(1, chips):
            chip_copy(k, i).wait_send()
        pair_copy(k).wait_send()


def per_device(tokens, norm_gain, router_weight, w_gate, w_up, w_down, selected):
    dp_count = lax.axis_size("dp")
    experts = lax.axis_size("expert")
    chips = dp_count // 2
    tok_rows, model_width = tokens.shape
    capacity = selected.shape[1]
    ff = w_gate.shape[2]
    slots = 4 * tok_rows // experts
    room = 3 * capacity // (2 * dp_count)
    half = experts // 2
    chunks = CHUNKS
    width = model_width // chunks
    all_rows = dp_count * room
    far = max(chips - 1, 1)
    in_any = pl.BlockSpec(memory_space=pl.ANY)
    dma = pltpu.SemaphoreType.DMA
    return pl.pallas_call(
        functools.partial(kernel, experts, chips, chunks),
        out_shape=jax.ShapeDtypeStruct((tok_rows, model_width), BF16),
        in_specs=[in_any] * 7,
        out_specs=pl.BlockSpec(memory_space=pltpu.VMEM),
        scratch_shapes=[
            pltpu.VMEM((tok_rows, model_width), BF16),
            pltpu.VMEM((1, model_width), BF16),
            pltpu.VMEM((experts, model_width), BF16),
            pltpu.VMEM((experts + 8, capacity), jnp.int32),
            pltpu.VMEM((2, tok_rows, half * slots), BF16),
            pltpu.VMEM((2, half * slots, tok_rows), BF16),
            pltpu.VMEM((room, experts * slots), BF16),
            pltpu.VMEM((experts * slots, room), BF16),
            pltpu.VMEM((2, tok_rows, half * slots), BF16),
            pltpu.VMEM((2, tok_rows, half * slots), BF16),
            pltpu.VMEM((chunks, tok_rows, width), BF16),
            pltpu.VMEM((chunks, tok_rows, width), BF16),
            pltpu.VMEM((chunks, 2, half, slots, width), BF16),
            pltpu.VMEM((chunks, experts, slots, width), BF16),
            pltpu.VMEM((chunks, dp_count, room, width), BF16),
            pltpu.VMEM((model_width, ff), BF16),
            pltpu.VMEM((model_width, ff), BF16),
            pltpu.VMEM((chunks, ff, width), BF16),
            pltpu.VMEM((all_rows, ff), F32),
            pltpu.VMEM((all_rows, ff), F32),
            pltpu.VMEM((all_rows, ff), BF16),
            pltpu.VMEM((chunks, chips, room, width), BF16),
            pltpu.VMEM((chunks, far, room, width), BF16),
            pltpu.VMEM((chunks, experts, slots, width), BF16),
            pltpu.VMEM((chunks, 2, half, slots, width), BF16),
            pltpu.VMEM((chunks, tok_rows, width), BF16),
            pltpu.VMEM((chunks, tok_rows, width), BF16),
            dma((4,)),
            dma((chunks, 2)),
            dma((chunks,)),
            dma((chunks,)),
            dma((chunks,)),
            dma((chunks, 2, half)),
            dma((chunks, experts)),
            dma((chunks, chips)),
            dma((chunks, chips)),
            dma((chunks, dp_count)),
            dma((chunks, chips)),
            dma((chunks, chips)),
            dma((chunks, far)),
            dma((chunks, far)),
            dma((chunks, experts)),
            dma((chunks, 2, half)),
            dma((chunks,)),
            dma((chunks,)),
        ],
        compiler_params=pltpu.CompilerParams(
            collective_id=0, has_side_effects=True, vmem_limit_bytes=63 * 2**20
        ),
        name="moe",
    )(
        tokens, norm_gain.reshape(1, model_width), router_weight.T, selected,
        w_gate[0], w_up[0], w_down[0],
    )


def solution(mesh):
    in_specs = (
        P(("dp", "expert"), None),
        P(),
        P(),
        P("expert", None, "dp"),
        P("expert", None, "dp"),
        P("expert", "dp", None),
        P(),
    )
    out_specs = P(("dp", "expert"), None)
    return jax.shard_map(
        per_device, mesh=mesh, in_specs=in_specs, out_specs=out_specs, check_vma=False
    )
```

```python
import functools

import jax
import jax.numpy as jnp
from jax import lax
from jax.experimental import pallas as pl
from jax.experimental.pallas import tpu as pltpu
from jax.sharding import PartitionSpec as P

MESH = pl.DeviceIdType.MESH
F32 = jnp.float32
BF16 = jnp.bfloat16
CHUNKS = 8
AHEAD = 2
OWN_SLOTS = 4
NEAR_LAG, CHIP_LAG, CORE_LAG = 2, 2, 1
SIB_LAG, X_LAG, BACK_LAG, PAIR_LAG = 1, 2, 2, 2


def tile_of(width):
    for tile in (256, 128):
        if width % tile == 0:
            return tile
    return width


def remote(src, dst, send_sem, recv_sem, **where):
    return pltpu.make_async_remote_copy(
        src_ref=src,
        dst_ref=dst,
        send_sem=send_sem,
        recv_sem=recv_sem,
        device_id=where,
        device_id_type=MESH,
    )


def iota(shape, axis):
    return lax.broadcasted_iota(jnp.int32, shape, axis)


def kernel(
    experts, chips, chunks,
    tokens_hbm, gain_hbm, router_hbm, selected_hbm, wg_hbm, wu_hbm, wd_hbm, out,
    tokens, gain, router, selected, chosen, pick, pack, unpack, mix_high, mix_low,
    tok_out, tok_in, outgoing, received, rows, wg, wu, wd, acc_g, acc_u, hidden,
    own, sib_in, x_in, returning, arrived, back_out, back_in,
    i_sem, w_sem, d_sem, t_send, t_recv, a_send, a_recv, x_send, s_send, b_recv,
    c_send, c_recv, o_send, o_recv, r_send, r_recv, p_send, p_recv,
):
    half = experts // 2
    tok_rows = tokens.shape[0]
    width = tok_out.shape[2]
    slots = received.shape[2]
    room = rows.shape[3]
    capacity = selected.shape[1]
    ff = wg.shape[1]
    tile = tile_of(ff)
    lanes = half * slots

    me = lax.axis_index("expert")
    dp = lax.axis_index("dp")
    chip, core = dp // 2, dp % 2
    base, local = (me // half) * half, me % half
    partner = (me + half) % experts
    sibling = 2 * chip + 1 - core

    loads = [
        pltpu.make_async_copy(src, dst, i_sem.at[i])
        for i, (src, dst) in enumerate(
            (
                (tokens_hbm, tokens),
                (gain_hbm, gain),
                (selected_hbm, selected.at[pl.ds(0, experts)]),
                (router_hbm, router),
            )
        )
    ]
    for copy in loads:
        copy.start()

    barrier = pltpu.get_barrier_semaphore()

    def expert_hello(i, carry):
        pl.semaphore_signal(
            barrier, inc=1, device_id={"expert": base + (local + i) % half}, device_id_type=MESH
        )
        return carry

    lax.fori_loop(1, half, expert_hello, 0)
    pl.semaphore_signal(barrier, inc=1, device_id={"expert": partner}, device_id_type=MESH)
    pl.semaphore_signal(barrier, inc=1, device_id={"dp": sibling}, device_id_type=MESH)
    for i in range(1, chips):
        pl.semaphore_signal(
            barrier,
            inc=1,
            device_id={"dp": 2 * ((chip + i) % chips) + core},
            device_id_type=MESH,
        )

    def weights(k):
        part = pl.ds(k * width, width)
        return (
            pltpu.make_async_copy(wg_hbm.at[part], wg.at[part], w_sem.at[k, 0]),
            pltpu.make_async_copy(wu_hbm.at[part], wu.at[part], w_sem.at[k, 1]),
        )

    def down_weights(k):
        part = pl.ds(k * width, width)
        return pltpu.make_async_copy(wd_hbm.at[:, part], wd.at[k], d_sem.at[k])

    loads[0].wait()
    loads[1].wait()
    for k in range(chunks):
        for copy in weights(k):
            copy.start()
    for k in range(chunks):
        down_weights(k).start()
    activations = tokens[...].astype(F32)
    mean_square = jnp.mean(activations * activations, axis=1, keepdims=True)
    scale = lax.rsqrt(mean_square + 1e-06)
    for k in range(chunks):
        part = slice(k * width, (k + 1) * width)
        tok_out[k] = (
            tokens[:, part].astype(F32) * scale * gain[part].reshape(1, width).astype(F32)
        ).astype(BF16)
    pl.semaphore_wait(barrier, half + chips)

    def to_partner(k):
        return remote(
            tok_out.at[k], tok_in.at[k], t_send.at[k], t_recv.at[k], expert=partner
        )

    def to_expert(k, side, i):
        near = (local + i) % half
        owner = (me + side * half) % experts
        return remote(
            outgoing.at[k, side, near], received.at[k, owner],
            a_send.at[k, side, near], a_recv.at[k, owner], expert=base + near,
        )

    def from_expert(k, side, i):
        near = (local + i) % half
        owner = (base + near + side * half) % experts
        return remote(
            outgoing.at[k, side, near], received.at[k, owner],
            a_send.at[k, side, near], a_recv.at[k, owner], expert=base + near,
        )

    def to_chip(k, i):
        other = 2 * ((chip + i) % chips) + core
        return remote(
            rows.at[k, core, chip], rows.at[k, core, chip],
            x_send.at[k, i], b_recv.at[k, core, chip], dp=other,
        )

    def from_chip(k, i):
        other = (chip + i) % chips
        return remote(
            rows.at[k, core, other], rows.at[k, core, other],
            x_send.at[k, i], b_recv.at[k, core, other], dp=2 * other + core,
        )

    def to_sibling(k, i):
        block = (chip + i) % chips
        return remote(
            rows.at[k, core, block], rows.at[k, core, block],
            s_send.at[k, i], b_recv.at[k, core, block], dp=sibling,
        )

    def from_sibling(k, i):
        block = (chip + i) % chips
        return remote(
            rows.at[k, 1 - core, block], rows.at[k, 1 - core, block],
            s_send.at[k, i], b_recv.at[k, 1 - core, block], dp=sibling,
        )

    @pl.when(core == 0)
    def _():
        for k in range(min(AHEAD, chunks)):
            to_partner(k).start()

    loads[2].wait()
    loads[3].wait()

    spot = iota((1, capacity), 1).astype(F32)
    lane = iota((1, lanes), 1).astype(F32)

    def choose(side):
        first = (dp * experts + (me + side * half) % experts) * tok_rows
        ids = first + iota((tok_rows, 1), 0)
        total = jnp.zeros((tok_rows, lanes), F32)
        for e in range(half):
            row = selected[pl.ds(base + e, 1), :]
            at = jnp.max(jnp.where(row == ids, spot, -1.0), axis=1, keepdims=True)
            begin = jnp.sum(jnp.where(row < first, 1.0, 0.0), axis=1, keepdims=True)
            goal = jnp.where(at >= 0.0, at - begin + float(e * slots), -1.0)
            total = total + jnp.where(goal == lane, 1.0, 0.0)
        chosen[side] = total.astype(BF16)
        pick[side] = total.T.astype(BF16)

    def send_rows(k, side, source):
        picked = jnp.dot(pick[side], source[k], preferred_element_type=F32)
        outgoing[k, side] = picked.astype(BF16).reshape(half, slots, width)

        def send(i, carry):
            to_expert(k, side, i).start()
            return carry

        lax.fori_loop(1, half, send, 0)
        received[k, (me + side * half) % experts] = outgoing[k, side, local]

    choose(0)

    @pl.when(core == 0)
    def _():
        send_rows(0, 0, tok_out)

    choose(1)

    mine = selected[pl.ds(me, 1), :]
    starts = (dp * experts + iota((experts + 8, 1), 0)) * tok_rows
    firsts = jnp.sum(jnp.where(mine < starts, 1.0, 0.0), axis=1, keepdims=True)
    place = iota((1, experts * slots), 1).astype(F32)
    target = jnp.full((1, experts * slots), -1.0, F32)
    slot = iota((slots, 1), 0).astype(F32)
    seats = iota((1, room), 1).astype(F32)
    for j in range(experts):
        offset = firsts[j : j + 1] - firsts[0:1]
        count = firsts[j + 1 : j + 2] - firsts[j : j + 1]
        within = place - float(j * slots)
        here = jnp.logical_and(within >= 0.0, within < count)
        target = jnp.where(here, within + offset, target)
        goal = jnp.where(slot < count, slot + offset, -1.0)
        unpack[j * slots : (j + 1) * slots, :] = jnp.where(goal == seats, 1.0, 0.0).astype(BF16)
    seat = iota((room, 1), 0).astype(F32)
    pack[...] = jnp.where(seat == target, 1.0, 0.0).astype(BF16)

    def weigh(side, source):
        logits = jnp.zeros((tok_rows, experts), F32)
        for k in range(chunks):
            logits = logits + lax.dot_general(
                source[k], router[:, k * width : (k + 1) * width],
                (((1,), (1,)), ((), ())), preferred_element_type=F32,
            )
        probs = jax.nn.sigmoid(logits)
        column = iota((1, experts), 1)
        spread = jnp.zeros((tok_rows, lanes), F32)
        for e in range(half):
            prob = jnp.sum(jnp.where(column == base + e, probs, 0.0), axis=1, keepdims=True)
            inside = jnp.logical_and(lane >= float(e * slots), lane < float((e + 1) * slots))
            spread = jnp.where(inside, prob, spread)
        mixing = jnp.where(chosen[side].astype(F32) > 0.5, spread, 0.0)
        high = mixing.astype(BF16)
        mix_high[side] = high
        mix_low[side] = (mixing - high.astype(F32)).astype(BF16)

    def sib_copy(k, i):
        return remote(
            rows.at[k, 1 - core, i], sib_in.at[k, i], c_send.at[k, i], c_recv.at[k, i], dp=sibling
        )

    def chip_copy(k, i):
        return remote(
            rows.at[k, core, i - 1], x_in.at[k, i - 1],
            o_send.at[k, i - 1], o_recv.at[k, i - 1],
            dp=2 * ((chip + i) % chips) + core,
        )

    def give_back(k, side, i):
        near = (local + i) % half
        owner = (base + near + side * half) % experts
        return remote(
            returning.at[k, owner], arrived.at[k, side, local],
            r_send.at[k, owner], r_recv.at[k, side, local], expert=base + near,
        )

    def take_back(k, side, i):
        near = (local + i) % half
        owner = (base + near + side * half) % experts
        return remote(
            returning.at[k, owner], arrived.at[k, side, near],
            r_send.at[k, owner], r_recv.at[k, side, near], expert=base + near,
        )

    def pair_copy(k):
        return remote(
            back_out.at[k], back_in.at[k], p_send.at[k], p_recv.at[k], expert=partner
        )

    def mixed(k, side):
        values = arrived[k, side].reshape(half * slots, width)
        sums = jnp.dot(mix_high[side], values, preferred_element_type=F32)
        return sums + jnp.dot(mix_low[side], values, preferred_element_type=F32)

    def take_side(k, side):
        def take(i, carry):
            take_back(k, side, i).wait_recv()
            return carry

        lax.fori_loop(1, half, take, 0)

    def when(k, *more):
        fits = jnp.logical_and(k >= 0, k < chunks)
        for condition in more:
            fits = jnp.logical_and(fits, condition)
        return pl.when(fits)

    lag_x = NEAR_LAG + CHIP_LAG
    lag_m = lag_x + CORE_LAG
    lag_w = lag_m + chunks
    lag_t = SIB_LAG + X_LAG
    lag_b = lag_t + BACK_LAG
    lag_p = lag_b + PAIR_LAG
    group_rows = chips * room

    def step(t, carry):
        s = t - core * chunks
        r = s - lag_w

        @when(s)
        def _():
            to_partner(s).wait_recv()
            send_rows(s, 1, tok_in)

        @when(s + AHEAD)
        def _():
            to_partner(s + AHEAD).start()

        @when(s + 1)
        def _():
            send_rows(s + 1, 0, tok_out)

        @when(s - NEAR_LAG)
        def _():
            k = s - NEAR_LAG

            def take(i, carry):
                from_expert(k, 0, i).wait_recv()
                from_expert(k, 1, i).wait_recv()
                return carry

            lax.fori_loop(1, half, take, 0)
            packed = jnp.dot(
                pack[...],
                received[k].reshape(experts * slots, width),
                preferred_element_type=F32,
            )
            rows[k, core, chip] = packed.astype(BF16)
            for i in range(1, chips):
                to_chip(k, i).start()
            to_sibling(k, 0).start()

        @when(s - lag_x)
        def _():
            k = s - lag_x
            for i in range(1, chips):
                from_chip(k, i).wait_recv()
                to_sibling(k, i).start()

        @when(r - SIB_LAG)
        def _():
            k = r - SIB_LAG
            for i in range(1, chips):
                to_chip(k, i).wait_send()
            for i in range(chips):
                to_sibling(k, i).wait_send()
            for i in range(chips):
                sib_copy(k, i).wait_recv()
            for i in range(1, chips):
                term = own[k % OWN_SLOTS, i] + sib_in[k, i].astype(F32)
                rows[k, core, i - 1] = term.astype(BF16)
                chip_copy(k, i).start()

        @when(r - lag_t)
        def _():
            k = r - lag_t
            total = own[k % OWN_SLOTS, 0] + sib_in[k, 0].astype(F32)
            for i in range(1, chips):
                chip_copy(k, i).wait_recv()
                total = total + x_in[k, i - 1].astype(F32)
            spread = jnp.dot(unpack[...], total.astype(BF16), preferred_element_type=F32)
            returning[k] = spread.astype(BF16).reshape(experts, slots, width)
            for side in (1, 0):

                def send(i, carry):
                    give_back(k, side, i).start()
                    return carry

                lax.fori_loop(1, half, send, 0)
                arrived[k, side, local] = returning[k, (me + side * half) % experts]

        @when(r - lag_b)
        def _():
            k = r - lag_b
            take_side(k, 1)
            back_out[k] = mixed(k, 1).astype(BF16)
            pair_copy(k).start()

        @when(r - lag_p)
        def _():
            k = r - lag_p
            take_side(k, 0)
            near_sum = mixed(k, 0)
            pair_copy(k).wait_recv()
            combined = near_sum + back_in[k].astype(F32)
            out[:, pl.ds(pl.multiple_of(k * width, width), width)] = combined.astype(BF16)

        @pl.when(s == chunks)
        def _():
            weigh(0, tok_out)
            weigh(1, tok_in)

        w = t - lag_w
        w_group, w_chunk = w // chunks, w % chunks

        @pl.when(jnp.logical_and(w >= 0, w < chunks))
        def _():
            down_weights(w_chunk).wait()

        def term_of(i):
            block = (chip + i) % chips
            part = pl.ds(pl.multiple_of(block * room, 16), room)
            return jnp.dot(hidden[w_group, part, :], wd[w_chunk], preferred_element_type=F32)

        @pl.when(jnp.logical_and(w >= 0, w_group == 1 - core))
        def _():
            def give(i, carry):
                rows[w_chunk, 1 - core, i] = term_of(i).astype(BF16)
                sib_copy(w_chunk, i).start()
                return carry

            lax.fori_loop(0, chips, give, 0)

        @pl.when(jnp.logical_and(w >= 0, w_group == core))
        def _():
            def keep(i, carry):
                own[w_chunk % OWN_SLOTS, i] = term_of(i)
                return carry

            lax.fori_loop(0, chips, keep, 0)

        m = t - lag_m
        group, k = m // chunks, m % chunks
        busy = jnp.logical_and(m >= 0, m < 2 * chunks)

        @pl.when(jnp.logical_and(busy, group == 1 - core))
        def _():
            for i in range(chips):
                from_sibling(k, i).wait_recv()

        @pl.when(jnp.logical_and(busy, group == 0))
        def _():
            for copy in weights(k):
                copy.wait()

        def multiply(first, last):
            def columns(n, carry):
                cols = pl.ds(pl.multiple_of(n * tile, tile), tile)
                depth = pl.ds(pl.multiple_of(k * width, width), width)
                block = rows[k, group].reshape(group_rows, width)
                g = jnp.dot(block, wg[depth, cols], preferred_element_type=F32)
                u = jnp.dot(block, wu[depth, cols], preferred_element_type=F32)
                if not first:
                    g = g + acc_g[:, cols]
                    u = u + acc_u[:, cols]
                if not last:
                    acc_g[:, cols] = g
                    acc_u[:, cols] = u
                else:
                    hidden[group, :, cols] = (jax.nn.gelu(g, approximate=True) * u).astype(BF16)
                return carry

            lax.fori_loop(0, ff // tile, columns, 0)

        @pl.when(jnp.logical_and(busy, k == 0))
        def _():
            multiply(True, chunks == 1)

        @pl.when(jnp.logical_and(busy, jnp.logical_and(k > 0, k < chunks - 1)))
        def _():
            multiply(False, False)

        @pl.when(jnp.logical_and(busy, jnp.logical_and(k > 0, k == chunks - 1)))
        def _():
            multiply(False, True)

        return carry

    lax.fori_loop(0, lag_w + 2 * chunks + lag_p, step, 0)

    def finish(k, carry):
        to_partner(k).wait_send()

        def sent(i, carry):
            for side in (0, 1):
                to_expert(k, side, i).wait_send()
                give_back(k, side, i).wait_send()
            return carry

        lax.fori_loop(1, half, sent, 0)
        for i in range(chips):
            sib_copy(k, i).wait_send()
        for i in range(1, chips):
            chip_copy(k, i).wait_send()
        pair_copy(k).wait_send()
        return carry

    lax.fori_loop(0, chunks, finish, 0)


def per_device(tokens, norm_gain, router_weight, w_gate, w_up, w_down, selected):
    dp_count = lax.axis_size("dp")
    experts = lax.axis_size("expert")
    chips = dp_count // 2
    tok_rows, model_width = tokens.shape
    capacity = selected.shape[1]
    ff = w_gate.shape[2]
    slots = 4 * tok_rows // experts
    room = 3 * capacity // (2 * dp_count)
    half = experts // 2
    chunks = CHUNKS
    width = model_width // chunks
    far = max(chips - 1, 1)
    in_any = pl.BlockSpec(memory_space=pl.ANY)
    dma = pltpu.SemaphoreType.DMA
    return pl.pallas_call(
        functools.partial(kernel, experts, chips, chunks),
        out_shape=jax.ShapeDtypeStruct((tok_rows, model_width), BF16),
        in_specs=[in_any] * 7,
        out_specs=pl.BlockSpec(memory_space=pltpu.VMEM),
        scratch_shapes=[
            pltpu.VMEM((tok_rows, model_width), BF16),
            pltpu.VMEM((model_width,), BF16),
            pltpu.VMEM((experts, model_width), BF16),
            pltpu.VMEM((experts + 8, capacity), jnp.int32),
            pltpu.VMEM((2, tok_rows, half * slots), BF16),
            pltpu.VMEM((2, half * slots, tok_rows), BF16),
            pltpu.VMEM((room, experts * slots), BF16),
            pltpu.VMEM((experts * slots, room), BF16),
            pltpu.VMEM((2, tok_rows, half * slots), BF16),
            pltpu.VMEM((2, tok_rows, half * slots), BF16),
            pltpu.VMEM((chunks, tok_rows, width), BF16),
            pltpu.VMEM((chunks, tok_rows, width), BF16),
            pltpu.VMEM((chunks, 2, half, slots, width), BF16),
            pltpu.VMEM((chunks, experts, slots, width), BF16),
            pltpu.VMEM((chunks, 2, chips, room, width), BF16),
            pltpu.VMEM((model_width, ff), BF16),
            pltpu.VMEM((model_width, ff), BF16),
            pltpu.VMEM((chunks, ff, width), BF16),
            pltpu.VMEM((chips * room, ff), F32),
            pltpu.VMEM((chips * room, ff), F32),
            pltpu.VMEM((2, chips * room, ff), BF16),
            pltpu.VMEM((OWN_SLOTS, chips, room, width), F32),
            pltpu.VMEM((chunks, chips, room, width), BF16),
            pltpu.VMEM((chunks, far, room, width), BF16),
            pltpu.VMEM((chunks, experts, slots, width), BF16),
            pltpu.VMEM((chunks, 2, half, slots, width), BF16),
            pltpu.VMEM((chunks, tok_rows, width), BF16),
            pltpu.VMEM((chunks, tok_rows, width), BF16),
            dma((4,)),
            dma((chunks, 2)),
            dma((chunks,)),
            dma((chunks,)),
            dma((chunks,)),
            dma((chunks, 2, half)),
            dma((chunks, experts)),
            dma((chunks, chips)),
            dma((chunks, chips)),
            dma((chunks, 2, chips)),
            dma((chunks, chips)),
            dma((chunks, chips)),
            dma((chunks, far)),
            dma((chunks, far)),
            dma((chunks, experts)),
            dma((chunks, 2, half)),
            dma((chunks,)),
            dma((chunks,)),
        ],
        compiler_params=pltpu.CompilerParams(
            collective_id=0, has_side_effects=True, vmem_limit_bytes=63 * 2**20
        ),
        name="moe",
    )(
        tokens, norm_gain, router_weight.T, selected,
        w_gate[0], w_up[0], w_down[0],
    )


def solution(mesh):
    in_specs = (
        P(("dp", "expert"), None),
        P(),
        P(),
        P("expert", None, "dp"),
        P("expert", None, "dp"),
        P("expert", "dp", None),
        P(),
    )
    out_specs = P(("dp", "expert"), None)
    return jax.shard_map(
        per_device, mesh=mesh, in_specs=in_specs, out_specs=out_specs, check_vma=False
    )
```

```python
import functools

import jax
import jax.numpy as jnp
from jax import lax
from jax.experimental import pallas as pl
from jax.experimental.pallas import tpu as pltpu
from jax.sharding import PartitionSpec as P

MESH = pl.DeviceIdType.MESH
F32 = jnp.float32
BF16 = jnp.bfloat16
CHUNKS = 8
AHEAD = 2
OWN_SLOTS = 4
NEAR_LAG, CHIP_LAG, CORE_LAG = 2, 2, 1
SIB_LAG, X_LAG, BACK_LAG, PAIR_LAG = 1, 2, 2, 3


def tile_of(width):
    for tile in (256, 128):
        if width % tile == 0:
            return tile
    return width


def remote(src, dst, send_sem, recv_sem, **where):
    return pltpu.make_async_remote_copy(
        src_ref=src,
        dst_ref=dst,
        send_sem=send_sem,
        recv_sem=recv_sem,
        device_id=where,
        device_id_type=MESH,
    )


def iota(shape, axis):
    return lax.broadcasted_iota(jnp.int32, shape, axis)


def kernel(
    experts, chips, chunks,
    tokens_hbm, gain_hbm, router_hbm, selected_hbm, wg_hbm, wu_hbm, wd_hbm, out,
    tokens, gain, router, selected, chosen, pick, pack, unpack, mix_high, mix_low,
    tok_out, tok_in, outgoing, received, rows, wg, wu, wd, acc_g, acc_u, hidden,
    own, sib_in, x_in, returning, arrived, back_out, back_in,
    i_sem, w_sem, d_sem, t_send, t_recv, a_send, a_recv, x_send, s_send, b_recv,
    c_send, c_recv, o_send, o_recv, r_send, r_recv, p_send, p_recv,
):
    half = experts // 2
    tok_rows = tokens.shape[0]
    width = tok_out.shape[2]
    slots = received.shape[2]
    room = rows.shape[3]
    capacity = selected.shape[1]
    ff = wg.shape[1]
    tile = tile_of(ff)
    lanes = half * slots

    me = lax.axis_index("expert")
    dp = lax.axis_index("dp")
    chip, core = dp // 2, dp % 2
    base, local = (me // half) * half, me % half
    partner = (me + half) % experts
    sibling = 2 * chip + 1 - core

    loads = [
        pltpu.make_async_copy(src, dst, i_sem.at[i])
        for i, (src, dst) in enumerate(
            (
                (tokens_hbm, tokens),
                (gain_hbm, gain),
                (selected_hbm, selected.at[pl.ds(0, experts)]),
                (router_hbm, router),
            )
        )
    ]
    for copy in loads:
        copy.start()

    barrier = pltpu.get_barrier_semaphore()

    def expert_hello(i, carry):
        pl.semaphore_signal(
            barrier, inc=1, device_id={"expert": base + (local + i) % half}, device_id_type=MESH
        )
        return carry

    lax.fori_loop(1, half, expert_hello, 0)
    pl.semaphore_signal(barrier, inc=1, device_id={"expert": partner}, device_id_type=MESH)
    pl.semaphore_signal(barrier, inc=1, device_id={"dp": sibling}, device_id_type=MESH)
    for i in range(1, chips):
        pl.semaphore_signal(
            barrier,
            inc=1,
            device_id={"dp": 2 * ((chip + i) % chips) + core},
            device_id_type=MESH,
        )

    def weights(k):
        part = pl.ds(k * width, width)
        return (
            pltpu.make_async_copy(wg_hbm.at[part], wg.at[part], w_sem.at[k, 0]),
            pltpu.make_async_copy(wu_hbm.at[part], wu.at[part], w_sem.at[k, 1]),
        )

    def down_weights(k):
        part = pl.ds(k * width, width)
        return pltpu.make_async_copy(wd_hbm.at[:, part], wd.at[k], d_sem.at[k])

    loads[0].wait()
    loads[1].wait()
    for k in range(chunks):
        for copy in weights(k):
            copy.start()
    for k in range(chunks):
        down_weights(k).start()
    activations = tokens[...].astype(F32)
    mean_square = jnp.mean(activations * activations, axis=1, keepdims=True)
    scale = lax.rsqrt(mean_square + 1e-06)
    for k in range(chunks):
        part = slice(k * width, (k + 1) * width)
        tok_out[k] = (
            tokens[:, part].astype(F32) * scale * gain[part].reshape(1, width).astype(F32)
        ).astype(BF16)
    pl.semaphore_wait(barrier, half + chips)

    def to_partner(k):
        return remote(
            tok_out.at[k], tok_in.at[k], t_send.at[k], t_recv.at[k], expert=partner
        )

    def to_expert(k, side, i):
        near = (local + i) % half
        owner = (me + side * half) % experts
        return remote(
            outgoing.at[k, side, near], received.at[k, owner],
            a_send.at[k, side, near], a_recv.at[k, owner], expert=base + near,
        )

    def from_expert(k, side, i):
        near = (local + i) % half
        owner = (base + near + side * half) % experts
        return remote(
            outgoing.at[k, side, near], received.at[k, owner],
            a_send.at[k, side, near], a_recv.at[k, owner], expert=base + near,
        )

    def to_chip(k, i):
        other = 2 * ((chip + i) % chips) + core
        return remote(
            rows.at[k, core, chip], rows.at[k, core, chip],
            x_send.at[k, i], b_recv.at[k, core, chip], dp=other,
        )

    def from_chip(k, i):
        other = (chip + i) % chips
        return remote(
            rows.at[k, core, other], rows.at[k, core, other],
            x_send.at[k, i], b_recv.at[k, core, other], dp=2 * other + core,
        )

    def to_sibling(k, i):
        block = (chip + i) % chips
        return remote(
            rows.at[k, core, block], rows.at[k, core, block],
            s_send.at[k, i], b_recv.at[k, core, block], dp=sibling,
        )

    def from_sibling(k, i):
        block = (chip + i) % chips
        return remote(
            rows.at[k, 1 - core, block], rows.at[k, 1 - core, block],
            s_send.at[k, i], b_recv.at[k, 1 - core, block], dp=sibling,
        )

    @pl.when(core == 1)
    def _():
        for k in range(min(AHEAD, chunks)):
            to_partner(k).start()

    loads[2].wait()
    loads[3].wait()

    spot = iota((1, capacity), 1).astype(F32)
    lane = iota((1, lanes), 1).astype(F32)

    def choose(side):
        first = (dp * experts + (me + side * half) % experts) * tok_rows
        ids = first + iota((tok_rows, 1), 0)
        total = jnp.zeros((tok_rows, lanes), F32)
        for e in range(half):
            row = selected[pl.ds(base + e, 1), :]
            at = jnp.max(jnp.where(row == ids, spot, -1.0), axis=1, keepdims=True)
            begin = jnp.sum(jnp.where(row < first, 1.0, 0.0), axis=1, keepdims=True)
            goal = jnp.where(at >= 0.0, at - begin + float(e * slots), -1.0)
            total = total + jnp.where(goal == lane, 1.0, 0.0)
        chosen[side] = total.astype(BF16)
        pick[side] = total.T.astype(BF16)

    def send_rows(k, side, source):
        picked = jnp.dot(pick[side], source[k], preferred_element_type=F32)
        outgoing[k, side] = picked.astype(BF16).reshape(half, slots, width)

        def send(i, carry):
            to_expert(k, side, i).start()
            return carry

        lax.fori_loop(1, half, send, 0)
        received[k, (me + side * half) % experts] = outgoing[k, side, local]

    choose(0)

    @pl.when(core == 1)
    def _():
        send_rows(0, 0, tok_out)

    choose(1)

    mine = selected[pl.ds(me, 1), :]
    starts = (dp * experts + iota((experts + 8, 1), 0)) * tok_rows
    firsts = jnp.sum(jnp.where(mine < starts, 1.0, 0.0), axis=1, keepdims=True)
    place = iota((1, experts * slots), 1).astype(F32)
    target = jnp.full((1, experts * slots), -1.0, F32)
    slot = iota((slots, 1), 0).astype(F32)
    seats = iota((1, room), 1).astype(F32)
    for j in range(experts):
        offset = firsts[j : j + 1] - firsts[0:1]
        count = firsts[j + 1 : j + 2] - firsts[j : j + 1]
        within = place - float(j * slots)
        here = jnp.logical_and(within >= 0.0, within < count)
        target = jnp.where(here, within + offset, target)
        goal = jnp.where(slot < count, slot + offset, -1.0)
        unpack[j * slots : (j + 1) * slots, :] = jnp.where(goal == seats, 1.0, 0.0).astype(BF16)
    seat = iota((room, 1), 0).astype(F32)
    pack[...] = jnp.where(seat == target, 1.0, 0.0).astype(BF16)

    def weigh(side, source):
        logits = jnp.zeros((tok_rows, experts), F32)
        for k in range(chunks):
            logits = logits + lax.dot_general(
                source[k], router[:, k * width : (k + 1) * width],
                (((1,), (1,)), ((), ())), preferred_element_type=F32,
            )
        probs = jax.nn.sigmoid(logits)
        column = iota((1, experts), 1)
        spread = jnp.zeros((tok_rows, lanes), F32)
        for e in range(half):
            prob = jnp.sum(jnp.where(column == base + e, probs, 0.0), axis=1, keepdims=True)
            inside = jnp.logical_and(lane >= float(e * slots), lane < float((e + 1) * slots))
            spread = jnp.where(inside, prob, spread)
        mixing = jnp.where(chosen[side].astype(F32) > 0.5, spread, 0.0)
        high = mixing.astype(BF16)
        mix_high[side] = high
        mix_low[side] = (mixing - high.astype(F32)).astype(BF16)

    def sib_copy(k, i):
        return remote(
            rows.at[k, 1 - core, i], sib_in.at[k, i], c_send.at[k, i], c_recv.at[k, i], dp=sibling
        )

    def chip_copy(k, i):
        return remote(
            rows.at[k, core, i - 1], x_in.at[k, i - 1],
            o_send.at[k, i - 1], o_recv.at[k, i - 1],
            dp=2 * ((chip + i) % chips) + core,
        )

    def give_back(k, side, i):
        near = (local + i) % half
        owner = (base + near + side * half) % experts
        return remote(
            returning.at[k, owner], arrived.at[k, side, local],
            r_send.at[k, owner], r_recv.at[k, side, local], expert=base + near,
        )

    def take_back(k, side, i):
        near = (local + i) % half
        owner = (base + near + side * half) % experts
        return remote(
            returning.at[k, owner], arrived.at[k, side, near],
            r_send.at[k, owner], r_recv.at[k, side, near], expert=base + near,
        )

    def pair_copy(k):
        return remote(
            back_out.at[k], back_in.at[k], p_send.at[k], p_recv.at[k], expert=partner
        )

    def mixed(k, side):
        values = arrived[k, side].reshape(half * slots, width)
        sums = jnp.dot(mix_high[side], values, preferred_element_type=F32)
        return sums + jnp.dot(mix_low[side], values, preferred_element_type=F32)

    def take_side(k, side):
        def take(i, carry):
            take_back(k, side, i).wait_recv()
            return carry

        lax.fori_loop(1, half, take, 0)

    def when(k, *more):
        fits = jnp.logical_and(k >= 0, k < chunks)
        for condition in more:
            fits = jnp.logical_and(fits, condition)
        return pl.when(fits)

    lag_x = NEAR_LAG + CHIP_LAG
    lag_m = lag_x + CORE_LAG
    lag_w = lag_m + chunks
    lag_t = SIB_LAG + X_LAG
    lag_b = lag_t + BACK_LAG
    lag_p = lag_b + PAIR_LAG
    group_rows = chips * room

    def step(t, carry):
        s = t - (1 - core) * chunks
        r = s - lag_w

        @when(s)
        def _():
            to_partner(s).wait_recv()
            send_rows(s, 1, tok_in)

        @when(s + AHEAD)
        def _():
            to_partner(s + AHEAD).start()

        @when(s + 1)
        def _():
            send_rows(s + 1, 0, tok_out)

        @when(s - NEAR_LAG)
        def _():
            k = s - NEAR_LAG

            def take(i, carry):
                from_expert(k, 0, i).wait_recv()
                from_expert(k, 1, i).wait_recv()
                return carry

            lax.fori_loop(1, half, take, 0)
            packed = jnp.dot(
                pack[...],
                received[k].reshape(experts * slots, width),
                preferred_element_type=F32,
            )
            rows[k, core, chip] = packed.astype(BF16)
            for i in range(1, chips):
                to_chip(k, i).start()
            to_sibling(k, 0).start()

        @when(s - lag_x)
        def _():
            k = s - lag_x
            for i in range(1, chips):
                from_chip(k, i).wait_recv()
                to_sibling(k, i).start()

        @when(r - SIB_LAG)
        def _():
            k = r - SIB_LAG
            for i in range(1, chips):
                to_chip(k, i).wait_send()
            for i in range(chips):
                to_sibling(k, i).wait_send()
            for i in range(chips):
                sib_copy(k, i).wait_recv()
            for i in range(1, chips):
                term = own[k % OWN_SLOTS, i] + sib_in[k, i].astype(F32)
                rows[k, core, i - 1] = term.astype(BF16)
                chip_copy(k, i).start()

        @when(r - lag_t)
        def _():
            k = r - lag_t
            total = own[k % OWN_SLOTS, 0] + sib_in[k, 0].astype(F32)
            for i in range(1, chips):
                chip_copy(k, i).wait_recv()
                total = total + x_in[k, i - 1].astype(F32)
            spread = jnp.dot(unpack[...], total.astype(BF16), preferred_element_type=F32)
            returning[k] = spread.astype(BF16).reshape(experts, slots, width)
            for side in (1, 0):

                def send(i, carry):
                    give_back(k, side, i).start()
                    return carry

                lax.fori_loop(1, half, send, 0)
                arrived[k, side, local] = returning[k, (me + side * half) % experts]

        @when(r - lag_b)
        def _():
            k = r - lag_b
            take_side(k, 1)
            back_out[k] = mixed(k, 1).astype(BF16)
            pair_copy(k).start()

        @when(r - lag_p)
        def _():
            k = r - lag_p
            take_side(k, 0)
            near_sum = mixed(k, 0)
            pair_copy(k).wait_recv()
            combined = near_sum + back_in[k].astype(F32)
            out[:, pl.ds(pl.multiple_of(k * width, width), width)] = combined.astype(BF16)

        @pl.when(s == chunks)
        def _():
            weigh(0, tok_out)
            weigh(1, tok_in)

        w = t - lag_w
        w_group, w_chunk = 1 - w // chunks, w % chunks

        @pl.when(jnp.logical_and(w >= 0, w < chunks))
        def _():
            down_weights(w_chunk).wait()

        def term_of(i):
            block = (chip + i) % chips
            part = pl.ds(pl.multiple_of(block * room, 16), room)
            return jnp.dot(hidden[w_group, part, :], wd[w_chunk], preferred_element_type=F32)

        @pl.when(jnp.logical_and(w >= 0, w_group == 1 - core))
        def _():
            def give(i, carry):
                rows[w_chunk, 1 - core, i] = term_of(i).astype(BF16)
                sib_copy(w_chunk, i).start()
                return carry

            lax.fori_loop(0, chips, give, 0)

        @pl.when(jnp.logical_and(w >= 0, w_group == core))
        def _():
            def keep(i, carry):
                own[w_chunk % OWN_SLOTS, i] = term_of(i)
                return carry

            lax.fori_loop(0, chips, keep, 0)

        m = t - lag_m
        turn, k = m // chunks, m % chunks
        group = 1 - turn
        busy = jnp.logical_and(m >= 0, m < 2 * chunks)

        @pl.when(jnp.logical_and(busy, group == 1 - core))
        def _():
            for i in range(chips):
                from_sibling(k, i).wait_recv()

        @pl.when(jnp.logical_and(busy, turn == 0))
        def _():
            for copy in weights(k):
                copy.wait()

        def multiply(first, last):
            def columns(n, carry):
                cols = pl.ds(pl.multiple_of(n * tile, tile), tile)
                depth = pl.ds(pl.multiple_of(k * width, width), width)
                block = rows[k, group].reshape(group_rows, width)
                g = jnp.dot(block, wg[depth, cols], preferred_element_type=F32)
                u = jnp.dot(block, wu[depth, cols], preferred_element_type=F32)
                if not first:
                    g = g + acc_g[:, cols]
                    u = u + acc_u[:, cols]
                if not last:
                    acc_g[:, cols] = g
                    acc_u[:, cols] = u
                else:
                    hidden[group, :, cols] = (jax.nn.gelu(g, approximate=True) * u).astype(BF16)
                return carry

            lax.fori_loop(0, ff // tile, columns, 0)

        @pl.when(jnp.logical_and(busy, k == 0))
        def _():
            multiply(True, chunks == 1)

        @pl.when(jnp.logical_and(busy, jnp.logical_and(k > 0, k < chunks - 1)))
        def _():
            multiply(False, False)

        @pl.when(jnp.logical_and(busy, jnp.logical_and(k > 0, k == chunks - 1)))
        def _():
            multiply(False, True)

        return carry

    lax.fori_loop(0, lag_w + 2 * chunks + lag_p, step, 0)

    def finish(k, carry):
        to_partner(k).wait_send()

        def sent(i, carry):
            for side in (0, 1):
                to_expert(k, side, i).wait_send()
                give_back(k, side, i).wait_send()
            return carry

        lax.fori_loop(1, half, sent, 0)
        for i in range(chips):
            sib_copy(k, i).wait_send()
        for i in range(1, chips):
            chip_copy(k, i).wait_send()
        pair_copy(k).wait_send()
        return carry

    lax.fori_loop(0, chunks, finish, 0)


def per_device(tokens, norm_gain, router_weight, w_gate, w_up, w_down, selected):
    dp_count = lax.axis_size("dp")
    experts = lax.axis_size("expert")
    chips = dp_count // 2
    tok_rows, model_width = tokens.shape
    capacity = selected.shape[1]
    ff = w_gate.shape[2]
    slots = 4 * tok_rows // experts
    room = 3 * capacity // (2 * dp_count)
    half = experts // 2
    chunks = CHUNKS
    width = model_width // chunks
    far = max(chips - 1, 1)
    in_any = pl.BlockSpec(memory_space=pl.ANY)
    dma = pltpu.SemaphoreType.DMA
    return pl.pallas_call(
        functools.partial(kernel, experts, chips, chunks),
        out_shape=jax.ShapeDtypeStruct((tok_rows, model_width), BF16),
        in_specs=[in_any] * 7,
        out_specs=pl.BlockSpec(memory_space=pltpu.VMEM),
        scratch_shapes=[
            pltpu.VMEM((tok_rows, model_width), BF16),
            pltpu.VMEM((model_width,), BF16),
            pltpu.VMEM((experts, model_width), BF16),
            pltpu.VMEM((experts + 8, capacity), jnp.int32),
            pltpu.VMEM((2, tok_rows, half * slots), BF16),
            pltpu.VMEM((2, half * slots, tok_rows), BF16),
            pltpu.VMEM((room, experts * slots), BF16),
            pltpu.VMEM((experts * slots, room), BF16),
            pltpu.VMEM((2, tok_rows, half * slots), BF16),
            pltpu.VMEM((2, tok_rows, half * slots), BF16),
            pltpu.VMEM((chunks, tok_rows, width), BF16),
            pltpu.VMEM((chunks, tok_rows, width), BF16),
            pltpu.VMEM((chunks, 2, half, slots, width), BF16),
            pltpu.VMEM((chunks, experts, slots, width), BF16),
            pltpu.VMEM((chunks, 2, chips, room, width), BF16),
            pltpu.VMEM((model_width, ff), BF16),
            pltpu.VMEM((model_width, ff), BF16),
            pltpu.VMEM((chunks, ff, width), BF16),
            pltpu.VMEM((chips * room, ff), F32),
            pltpu.VMEM((chips * room, ff), F32),
            pltpu.VMEM((2, chips * room, ff), BF16),
            pltpu.VMEM((OWN_SLOTS, chips, room, width), F32),
            pltpu.VMEM((chunks, chips, room, width), BF16),
            pltpu.VMEM((chunks, far, room, width), BF16),
            pltpu.VMEM((chunks, experts, slots, width), BF16),
            pltpu.VMEM((chunks, 2, half, slots, width), BF16),
            pltpu.VMEM((chunks, tok_rows, width), BF16),
            pltpu.VMEM((chunks, tok_rows, width), BF16),
            dma((4,)),
            dma((chunks, 2)),
            dma((chunks,)),
            dma((chunks,)),
            dma((chunks,)),
            dma((chunks, 2, half)),
            dma((chunks, experts)),
            dma((chunks, chips)),
            dma((chunks, chips)),
            dma((chunks, 2, chips)),
            dma((chunks, chips)),
            dma((chunks, chips)),
            dma((chunks, far)),
            dma((chunks, far)),
            dma((chunks, experts)),
            dma((chunks, 2, half)),
            dma((chunks,)),
            dma((chunks,)),
        ],
        compiler_params=pltpu.CompilerParams(
            collective_id=0, has_side_effects=True, vmem_limit_bytes=63 * 2**20
        ),
        name="moe",
    )(
        tokens, norm_gain, router_weight.T, selected,
        w_gate[0], w_up[0], w_down[0],
    )


def solution(mesh):
    in_specs = (
        P(("dp", "expert"), None),
        P(),
        P(),
        P("expert", None, "dp"),
        P("expert", None, "dp"),
        P("expert", "dp", None),
        P(),
    )
    out_specs = P(("dp", "expert"), None)
    return jax.shard_map(
        per_device, mesh=mesh, in_specs=in_specs, out_specs=out_specs, check_vma=False
    )
```

```python
import functools

import jax
import jax.numpy as jnp
from jax import lax
from jax.experimental import pallas as pl
from jax.experimental.pallas import tpu as pltpu
from jax.sharding import PartitionSpec as P

MESH = pl.DeviceIdType.MESH
F32 = jnp.float32
BF16 = jnp.bfloat16
CHUNKS = 8
AHEAD = 2
OWN_SLOTS = 4
NEAR_LAG, CHIP_LAG, CORE_LAG = 2, 2, 1
SIB_LAG, X_LAG, BACK_LAG, PAIR_LAG = 1, 2, 2, 3


def tile_of(width):
    for tile in (256, 128):
        if width % tile == 0:
            return tile
    return width


def remote(src, dst, send_sem, recv_sem, **where):
    return pltpu.make_async_remote_copy(
        src_ref=src,
        dst_ref=dst,
        send_sem=send_sem,
        recv_sem=recv_sem,
        device_id=where,
        device_id_type=MESH,
    )


def iota(shape, axis):
    return lax.broadcasted_iota(jnp.int32, shape, axis)


def kernel(
    experts, chips, chunks,
    tokens_hbm, gain_hbm, router_hbm, selected_hbm, wg_hbm, wu_hbm, wd_hbm, out,
    tokens, gain, router, selected, chosen, pick, pack, unpack, mix_high, mix_low,
    tok_out, tok_in, outgoing, received, rows, wg, wu, wd, acc_g, acc_u, hidden,
    own, sib_in, x_in, returning, arrived, back_out, back_in,
    i_sem, w_sem, d_sem, t_send, t_recv, a_send, a_recv, x_send, s_send, b_recv,
    c_send, c_recv, o_send, o_recv, r_send, r_recv, p_send, p_recv,
):
    half = experts // 2
    tok_rows = tokens.shape[0]
    width = tok_out.shape[2]
    slots = received.shape[2]
    room = rows.shape[3]
    capacity = selected.shape[1]
    ff = wg.shape[1]
    tile = tile_of(ff)
    lanes = half * slots

    me = lax.axis_index("expert")
    dp = lax.axis_index("dp")
    chip, core = dp // 2, dp % 2
    base, local = (me // half) * half, me % half
    partner = (me + half) % experts
    sibling = 2 * chip + 1 - core

    loads = [
        pltpu.make_async_copy(src, dst, i_sem.at[i])
        for i, (src, dst) in enumerate(
            (
                (tokens_hbm, tokens),
                (gain_hbm, gain),
                (selected_hbm, selected.at[pl.ds(0, experts)]),
                (router_hbm, router),
            )
        )
    ]
    for copy in loads:
        copy.start()

    barrier = pltpu.get_barrier_semaphore()

    def expert_hello(i, carry):
        pl.semaphore_signal(
            barrier, inc=1, device_id={"expert": base + (local + i) % half}, device_id_type=MESH
        )
        return carry

    lax.fori_loop(1, half, expert_hello, 0)
    pl.semaphore_signal(barrier, inc=1, device_id={"expert": partner}, device_id_type=MESH)
    pl.semaphore_signal(barrier, inc=1, device_id={"dp": sibling}, device_id_type=MESH)
    for i in range(1, chips):
        pl.semaphore_signal(
            barrier,
            inc=1,
            device_id={"dp": 2 * ((chip + i) % chips) + core},
            device_id_type=MESH,
        )

    def weights(k):
        part = pl.ds(k * width, width)
        return (
            pltpu.make_async_copy(wg_hbm.at[part], wg.at[part], w_sem.at[k, 0]),
            pltpu.make_async_copy(wu_hbm.at[part], wu.at[part], w_sem.at[k, 1]),
        )

    def down_weights(k):
        part = pl.ds(k * width, width)
        return pltpu.make_async_copy(wd_hbm.at[:, part], wd.at[k], d_sem.at[k])

    loads[0].wait()
    loads[1].wait()
    for k in range(chunks):
        for copy in weights(k):
            copy.start()
    for k in range(chunks):
        down_weights(k).start()
    activations = tokens[...].astype(F32)
    mean_square = jnp.mean(activations * activations, axis=1, keepdims=True)
    scale = lax.rsqrt(mean_square + 1e-06)
    for k in range(chunks):
        part = slice(k * width, (k + 1) * width)
        tok_out[k] = (
            tokens[:, part].astype(F32) * scale * gain[part].reshape(1, width).astype(F32)
        ).astype(BF16)
    pl.semaphore_wait(barrier, half + chips)

    def to_partner(k):
        return remote(
            tok_out.at[k], tok_in.at[k], t_send.at[k], t_recv.at[k], expert=partner
        )

    def to_expert(k, side, i):
        near = (local + i) % half
        owner = (me + side * half) % experts
        return remote(
            outgoing.at[k, side, near], received.at[k, owner],
            a_send.at[k, side, near], a_recv.at[k, owner], expert=base + near,
        )

    def from_expert(k, side, i):
        near = (local + i) % half
        owner = (base + near + side * half) % experts
        return remote(
            outgoing.at[k, side, near], received.at[k, owner],
            a_send.at[k, side, near], a_recv.at[k, owner], expert=base + near,
        )

    def to_chip(k, i):
        other = 2 * ((chip + i) % chips) + core
        return remote(
            rows.at[k, core, chip], rows.at[k, core, chip],
            x_send.at[k, i], b_recv.at[k, core, chip], dp=other,
        )

    def from_chip(k, i):
        other = (chip + i) % chips
        return remote(
            rows.at[k, core, other], rows.at[k, core, other],
            x_send.at[k, i], b_recv.at[k, core, other], dp=2 * other + core,
        )

    def to_sibling(k, i):
        block = (chip + i) % chips
        return remote(
            rows.at[k, core, block], rows.at[k, core, block],
            s_send.at[k, i], b_recv.at[k, core, block], dp=sibling,
        )

    def from_sibling(k, i):
        block = (chip + i) % chips
        return remote(
            rows.at[k, 1 - core, block], rows.at[k, 1 - core, block],
            s_send.at[k, i], b_recv.at[k, 1 - core, block], dp=sibling,
        )

    @pl.when(core == 1)
    def _():
        for k in range(min(AHEAD, chunks)):
            to_partner(k).start()

    loads[2].wait()
    loads[3].wait()

    spot = iota((1, capacity), 1).astype(F32)
    lane = iota((1, lanes), 1).astype(F32)

    def choose(side):
        first = (dp * experts + (me + side * half) % experts) * tok_rows
        ids = first + iota((tok_rows, 1), 0)
        total = jnp.zeros((tok_rows, lanes), F32)
        for e in range(half):
            row = selected[pl.ds(base + e, 1), :]
            at = jnp.max(jnp.where(row == ids, spot, -1.0), axis=1, keepdims=True)
            begin = jnp.sum(jnp.where(row < first, 1.0, 0.0), axis=1, keepdims=True)
            goal = jnp.where(at >= 0.0, at - begin + float(e * slots), -1.0)
            total = total + jnp.where(goal == lane, 1.0, 0.0)
        chosen[side] = total.astype(BF16)
        pick[side] = total.T.astype(BF16)

    def send_rows(k, side, source):
        picked = jnp.dot(pick[side], source[k], preferred_element_type=F32)
        outgoing[k, side] = picked.astype(BF16).reshape(half, slots, width)

        def send(i, carry):
            to_expert(k, side, i).start()
            return carry

        lax.fori_loop(1, half, send, 0)
        received[k, (me + side * half) % experts] = outgoing[k, side, local]

    choose(0)

    @pl.when(core == 1)
    def _():
        send_rows(0, 0, tok_out)

    choose(1)

    mine = selected[pl.ds(me, 1), :]
    starts = (dp * experts + iota((experts + 8, 1), 0)) * tok_rows
    firsts = jnp.sum(jnp.where(mine < starts, 1.0, 0.0), axis=1, keepdims=True)
    place = iota((1, experts * slots), 1).astype(F32)
    target = jnp.full((1, experts * slots), -1.0, F32)
    for j in range(experts):
        offset = firsts[j : j + 1] - firsts[0:1]
        count = firsts[j + 1 : j + 2] - firsts[j : j + 1]
        within = place - float(j * slots)
        here = jnp.logical_and(within >= 0.0, within < count)
        target = jnp.where(here, within + offset, target)
    seat = iota((room, 1), 0).astype(F32)
    pack[...] = jnp.where(seat == target, 1.0, 0.0).astype(BF16)

    def place_back():
        slot = iota((slots, 1), 0).astype(F32)
        seats = iota((1, room), 1).astype(F32)
        for j in range(experts):
            offset = firsts[j : j + 1] - firsts[0:1]
            count = firsts[j + 1 : j + 2] - firsts[j : j + 1]
            goal = jnp.where(slot < count, slot + offset, -1.0)
            part = slice(j * slots, (j + 1) * slots)
            unpack[part, :] = jnp.where(goal == seats, 1.0, 0.0).astype(BF16)

    def weigh(side, source):
        logits = jnp.zeros((tok_rows, experts), F32)
        for k in range(chunks):
            logits = logits + lax.dot_general(
                source[k], router[:, k * width : (k + 1) * width],
                (((1,), (1,)), ((), ())), preferred_element_type=F32,
            )
        probs = jax.nn.sigmoid(logits)
        column = iota((1, experts), 1)
        spread = jnp.zeros((tok_rows, lanes), F32)
        for e in range(half):
            prob = jnp.sum(jnp.where(column == base + e, probs, 0.0), axis=1, keepdims=True)
            inside = jnp.logical_and(lane >= float(e * slots), lane < float((e + 1) * slots))
            spread = jnp.where(inside, prob, spread)
        mixing = jnp.where(chosen[side].astype(F32) > 0.5, spread, 0.0)
        high = mixing.astype(BF16)
        mix_high[side] = high
        mix_low[side] = (mixing - high.astype(F32)).astype(BF16)

    def sib_copy(k, i):
        return remote(
            rows.at[k, 1 - core, i], sib_in.at[k, i], c_send.at[k, i], c_recv.at[k, i], dp=sibling
        )

    def chip_copy(k, i):
        return remote(
            rows.at[k, core, i - 1], x_in.at[k, i - 1],
            o_send.at[k, i - 1], o_recv.at[k, i - 1],
            dp=2 * ((chip + i) % chips) + core,
        )

    def give_back(k, side, i):
        near = (local + i) % half
        owner = (base + near + side * half) % experts
        return remote(
            returning.at[k, owner], arrived.at[k, side, local],
            r_send.at[k, owner], r_recv.at[k, side, local], expert=base + near,
        )

    def take_back(k, side, i):
        near = (local + i) % half
        owner = (base + near + side * half) % experts
        return remote(
            returning.at[k, owner], arrived.at[k, side, near],
            r_send.at[k, owner], r_recv.at[k, side, near], expert=base + near,
        )

    def pair_copy(k):
        return remote(
            back_out.at[k], back_in.at[k], p_send.at[k], p_recv.at[k], expert=partner
        )

    def mixed(k, side):
        values = arrived[k, side].reshape(half * slots, width)
        sums = jnp.dot(mix_high[side], values, preferred_element_type=F32)
        return sums + jnp.dot(mix_low[side], values, preferred_element_type=F32)

    def take_side(k, side):
        def take(i, carry):
            take_back(k, side, i).wait_recv()
            return carry

        lax.fori_loop(1, half, take, 0)

    def when(k, *more):
        fits = jnp.logical_and(k >= 0, k < chunks)
        for condition in more:
            fits = jnp.logical_and(fits, condition)
        return pl.when(fits)

    lag_x = NEAR_LAG + CHIP_LAG
    lag_m = lag_x + CORE_LAG
    lag_w = lag_m + chunks
    lag_t = SIB_LAG + X_LAG
    lag_b = lag_t + BACK_LAG
    lag_p = lag_b + PAIR_LAG
    group_rows = chips * room

    def step(t, carry):
        s = t - (1 - core) * chunks
        r = s - lag_w

        @when(s + AHEAD)
        def _():
            to_partner(s + AHEAD).start()

        @when(s + 1)
        def _():
            send_rows(s + 1, 0, tok_out)

        @when(s - NEAR_LAG)
        def _():
            k = s - NEAR_LAG

            def take(i, carry):
                from_expert(k, 0, i).wait_recv()
                from_expert(k, 1, i).wait_recv()
                return carry

            lax.fori_loop(1, half, take, 0)
            packed = jnp.dot(
                pack[...],
                received[k].reshape(experts * slots, width),
                preferred_element_type=F32,
            )
            rows[k, core, chip] = packed.astype(BF16)
            for i in range(1, chips):
                to_chip(k, i).start()
            to_sibling(k, 0).start()

        @when(s - lag_x)
        def _():
            k = s - lag_x
            for i in range(1, chips):
                from_chip(k, i).wait_recv()
                to_sibling(k, i).start()

        @when(s)
        def _():
            to_partner(s).wait_recv()
            send_rows(s, 1, tok_in)

        @when(r - SIB_LAG)
        def _():
            k = r - SIB_LAG
            for i in range(1, chips):
                to_chip(k, i).wait_send()
            for i in range(chips):
                to_sibling(k, i).wait_send()
            for i in range(chips):
                sib_copy(k, i).wait_recv()
            for i in range(1, chips):
                term = own[k % OWN_SLOTS, i] + sib_in[k, i].astype(F32)
                rows[k, core, i - 1] = term.astype(BF16)
                chip_copy(k, i).start()

        @when(r - lag_t)
        def _():
            k = r - lag_t
            total = own[k % OWN_SLOTS, 0] + sib_in[k, 0].astype(F32)
            for i in range(1, chips):
                chip_copy(k, i).wait_recv()
                total = total + x_in[k, i - 1].astype(F32)
            spread = jnp.dot(unpack[...], total.astype(BF16), preferred_element_type=F32)
            returning[k] = spread.astype(BF16).reshape(experts, slots, width)
            for side in (1, 0):

                def send(i, carry):
                    give_back(k, side, i).start()
                    return carry

                lax.fori_loop(1, half, send, 0)
                arrived[k, side, local] = returning[k, (me + side * half) % experts]

        @when(r - lag_b)
        def _():
            k = r - lag_b
            take_side(k, 1)
            back_out[k] = mixed(k, 1).astype(BF16)
            pair_copy(k).start()

        @when(r - lag_p)
        def _():
            k = r - lag_p
            take_side(k, 0)
            near_sum = mixed(k, 0)
            pair_copy(k).wait_recv()
            combined = near_sum + back_in[k].astype(F32)
            out[:, pl.ds(pl.multiple_of(k * width, width), width)] = combined.astype(BF16)

        @pl.when(s == chunks)
        def _():
            place_back()
            weigh(0, tok_out)
            weigh(1, tok_in)

        w = t - lag_w
        w_group, w_chunk = 1 - w // chunks, w % chunks

        @pl.when(jnp.logical_and(w >= 0, w < chunks))
        def _():
            down_weights(w_chunk).wait()

        def term_of(i):
            block = (chip + i) % chips
            part = pl.ds(pl.multiple_of(block * room, 16), room)
            return jnp.dot(hidden[w_group, part, :], wd[w_chunk], preferred_element_type=F32)

        @pl.when(jnp.logical_and(w >= 0, w_group == 1 - core))
        def _():
            def give(i, carry):
                rows[w_chunk, 1 - core, i] = term_of(i).astype(BF16)
                sib_copy(w_chunk, i).start()
                return carry

            lax.fori_loop(0, chips, give, 0)

        @pl.when(jnp.logical_and(w >= 0, w_group == core))
        def _():
            def keep(i, carry):
                own[w_chunk % OWN_SLOTS, i] = term_of(i)
                return carry

            lax.fori_loop(0, chips, keep, 0)

        m = t - lag_m
        turn, k = m // chunks, m % chunks
        group = 1 - turn
        busy = jnp.logical_and(m >= 0, m < 2 * chunks)

        @pl.when(jnp.logical_and(busy, group == 1 - core))
        def _():
            for i in range(chips):
                from_sibling(k, i).wait_recv()

        @pl.when(jnp.logical_and(busy, turn == 0))
        def _():
            for copy in weights(k):
                copy.wait()

        def multiply(first, last):
            def columns(n, carry):
                cols = pl.ds(pl.multiple_of(n * tile, tile), tile)
                depth = pl.ds(pl.multiple_of(k * width, width), width)
                block = rows[k, group].reshape(group_rows, width)
                g = jnp.dot(block, wg[depth, cols], preferred_element_type=F32)
                u = jnp.dot(block, wu[depth, cols], preferred_element_type=F32)
                if not first:
                    g = g + acc_g[:, cols]
                    u = u + acc_u[:, cols]
                if not last:
                    acc_g[:, cols] = g
                    acc_u[:, cols] = u
                else:
                    hidden[group, :, cols] = (jax.nn.gelu(g, approximate=True) * u).astype(BF16)
                return carry

            lax.fori_loop(0, ff // tile, columns, 0)

        @pl.when(jnp.logical_and(busy, k == 0))
        def _():
            multiply(True, chunks == 1)

        @pl.when(jnp.logical_and(busy, jnp.logical_and(k > 0, k < chunks - 1)))
        def _():
            multiply(False, False)

        @pl.when(jnp.logical_and(busy, jnp.logical_and(k > 0, k == chunks - 1)))
        def _():
            multiply(False, True)

        return carry

    lax.fori_loop(0, lag_w + 2 * chunks + lag_p, step, 0)

    def finish(k, carry):
        to_partner(k).wait_send()

        def sent(i, carry):
            for side in (0, 1):
                to_expert(k, side, i).wait_send()
                give_back(k, side, i).wait_send()
            return carry

        lax.fori_loop(1, half, sent, 0)
        for i in range(chips):
            sib_copy(k, i).wait_send()
        for i in range(1, chips):
            chip_copy(k, i).wait_send()
        pair_copy(k).wait_send()
        return carry

    lax.fori_loop(0, chunks, finish, 0)


def per_device(tokens, norm_gain, router_weight, w_gate, w_up, w_down, selected):
    dp_count = lax.axis_size("dp")
    experts = lax.axis_size("expert")
    chips = dp_count // 2
    tok_rows, model_width = tokens.shape
    capacity = selected.shape[1]
    ff = w_gate.shape[2]
    slots = 4 * tok_rows // experts
    room = 3 * capacity // (2 * dp_count)
    half = experts // 2
    chunks = CHUNKS
    width = model_width // chunks
    far = max(chips - 1, 1)
    in_any = pl.BlockSpec(memory_space=pl.ANY)
    dma = pltpu.SemaphoreType.DMA
    return pl.pallas_call(
        functools.partial(kernel, experts, chips, chunks),
        out_shape=jax.ShapeDtypeStruct((tok_rows, model_width), BF16),
        in_specs=[in_any] * 7,
        out_specs=pl.BlockSpec(memory_space=pltpu.VMEM),
        scratch_shapes=[
            pltpu.VMEM((tok_rows, model_width), BF16),
            pltpu.VMEM((model_width,), BF16),
            pltpu.VMEM((experts, model_width), BF16),
            pltpu.VMEM((experts + 8, capacity), jnp.int32),
            pltpu.VMEM((2, tok_rows, half * slots), BF16),
            pltpu.VMEM((2, half * slots, tok_rows), BF16),
            pltpu.VMEM((room, experts * slots), BF16),
            pltpu.VMEM((experts * slots, room), BF16),
            pltpu.VMEM((2, tok_rows, half * slots), BF16),
            pltpu.VMEM((2, tok_rows, half * slots), BF16),
            pltpu.VMEM((chunks, tok_rows, width), BF16),
            pltpu.VMEM((chunks, tok_rows, width), BF16),
            pltpu.VMEM((chunks, 2, half, slots, width), BF16),
            pltpu.VMEM((chunks, experts, slots, width), BF16),
            pltpu.VMEM((chunks, 2, chips, room, width), BF16),
            pltpu.VMEM((model_width, ff), BF16),
            pltpu.VMEM((model_width, ff), BF16),
            pltpu.VMEM((chunks, ff, width), BF16),
            pltpu.VMEM((chips * room, ff), F32),
            pltpu.VMEM((chips * room, ff), F32),
            pltpu.VMEM((2, chips * room, ff), BF16),
            pltpu.VMEM((OWN_SLOTS, chips, room, width), F32),
            pltpu.VMEM((chunks, chips, room, width), BF16),
            pltpu.VMEM((chunks, far, room, width), BF16),
            pltpu.VMEM((chunks, experts, slots, width), BF16),
            pltpu.VMEM((chunks, 2, half, slots, width), BF16),
            pltpu.VMEM((chunks, tok_rows, width), BF16),
            pltpu.VMEM((chunks, tok_rows, width), BF16),
            dma((4,)),
            dma((chunks, 2)),
            dma((chunks,)),
            dma((chunks,)),
            dma((chunks,)),
            dma((chunks, 2, half)),
            dma((chunks, experts)),
            dma((chunks, chips)),
            dma((chunks, chips)),
            dma((chunks, 2, chips)),
            dma((chunks, chips)),
            dma((chunks, chips)),
            dma((chunks, far)),
            dma((chunks, far)),
            dma((chunks, experts)),
            dma((chunks, 2, half)),
            dma((chunks,)),
            dma((chunks,)),
        ],
        compiler_params=pltpu.CompilerParams(
            collective_id=0, has_side_effects=True, vmem_limit_bytes=63 * 2**20
        ),
        name="moe",
    )(
        tokens, norm_gain, router_weight.T, selected,
        w_gate[0], w_up[0], w_down[0],
    )


def solution(mesh):
    in_specs = (
        P(("dp", "expert"), None),
        P(),
        P(),
        P("expert", None, "dp"),
        P("expert", None, "dp"),
        P("expert", "dp", None),
        P(),
    )
    out_specs = P(("dp", "expert"), None)
    return jax.shard_map(
        per_device, mesh=mesh, in_specs=in_specs, out_specs=out_specs, check_vma=False
    )
```
